32 devices in a mesh: wide: 8 (over z, core), narrow: 4 (over y, x).
Axes of the slice: x: 2, y: 2, z: 4, core: 2. Of those that a mesh axis runs over, the one named last changes fastest.
Arguments:
- offsets: float32 [2, 8, 4, 8192], P(None, 'wide', 'narrow'), may hold values from -1 to 1
- strengths: float32 [2, 8, 4, 8192], P(None, 'wide', 'narrow'), may hold values from -1.2 to 1.2
- leaf_map: int32 [8, 4, 8192], P('wide', 'narrow'), may hold values from 0 to 1023
- shift_matrices: float32 [7, 4, 128, 128], replicated, may hold values from -0.25 to 0.25
- transfer_diagonal: float32 [5, 49, 128], replicated, may hold values from -1.25 to 1.25
Outputs:
- leaf_multipoles: float32 [256, 128, 128], P('wide', 'narrow')
- local_zero: float32 [8, 4, 128], P('wide', 'narrow')
- local_one: float32 [16, 8, 128], P('wide', 'narrow')
- local_two: float32 [32, 16, 128], P('wide', 'narrow')
- local_three: float32 [64, 32, 128], P('wide', 'narrow')
- coarse_local: float32 [4, 2, 128], replicated
- top_multipole: float32 [2, 1, 128], replicated
The draws below stay inside these ranges and needn't reach their ends.
All inputs are finite; a program needn't handle non-finite values.
Results may differ from the reference program's by a relative error of at most 0.0003.
Values sent between devices are 32-bit elements; how exact they have to be, the bound alone decides.
A program may use at most 128 MiB of HBM per device.

```python
import math
import jax
import jax.numpy as jnp
from jax import lax

ORDER = 64
COEFFS = 128
LOCAL = 5
COARSE = 2
LEAF_SIDE = 32
TRANSFER_LEVELS = 5
PAN_DEV = 8192
N_WIDE = 8
N_NARROW = 4


def set_ends(drawn, key, low, top_value):
    longest = drawn.shape.index(max(drawn.shape))
    spots = []
    for shift in (0, 1):
        where = [jax.random.randint(jax.random.fold_in(key, axis), (), 0, length) for axis, length in enumerate(drawn.shape)]
        where[longest] = (where[longest] + shift) % drawn.shape[longest]
        spots.append(tuple(where))
    return drawn.at[spots[0]].set(low).at[spots[1]].set(top_value)


def shard_levels(stream_key, shape, split, low, high):
    gain, own = 1.0, jax.random.fold_in(stream_key, 6)
    for position, blocks in split:
        steps = jnp.exp(jax.random.uniform(jax.random.fold_in(own, position), (blocks,), jnp.float32, low / len(split), high / len(split)))
        gain = gain * jnp.repeat(steps, shape[position] // blocks).reshape([-1 if axis == position else 1 for axis in range(len(shape))])
    return gain


def centred(key, dims, scale, reach, cuts=(), held_as=jnp.bfloat16):
    entries = jax.random.normal(key, dims, jnp.float32) * scale
    if len(cuts) > 0:
        entries = shard_levels(key, dims, cuts, -0.22, 0.18) * entries
    return jnp.clip(entries, min=-reach, max=reach).astype(held_as)


def setup_inputs(seed: int = 0) -> dict:
    splits = jax.random.split(jax.random.key(seed), 6)
    return {
        "offsets": jnp.clip(jax.random.uniform(splits[0], (2, N_WIDE, N_NARROW, PAN_DEV), jnp.float32, -1.0, 1.0) * shard_levels(splits[0], (2, N_WIDE, N_NARROW, PAN_DEV), ((1, 8), (2, 4)), -0.4, 0.0), -1.0, 1.0),
        "strengths": centred(splits[1], (2, N_WIDE, N_NARROW, PAN_DEV), 0.2, 1.2, ((1, 8), (2, 4)), jnp.float32),
        "leaf_map": set_ends(jax.random.randint(splits[2], (N_WIDE, N_NARROW, PAN_DEV), 0, LEAF_SIDE * LEAF_SIDE), jax.random.fold_in(splits[2], 1), 0, (LEAF_SIDE * LEAF_SIDE) - 1).astype(jnp.int32),
        "shift_matrices": centred(splits[3], (LOCAL + COARSE, 4, COEFFS, COEFFS), (4 * COEFFS) ** -0.5, 0.25, (), jnp.float32),
        "transfer_diagonal": centred(splits[4], (TRANSFER_LEVELS, 49, COEFFS), 0.2, 1.25, (), jnp.float32),
    }


HIGHEST = lax.Precision.HIGHEST


def panel_terms(coords, charge):
    degree = jnp.arange(ORDER).astype(jnp.float32)
    cheb_first = jnp.cos(degree[None, :] * jnp.arccos(coords[0])[:, None])
    cheb_second = jnp.cos(degree[None, :] * jnp.arccos(coords[1])[:, None])
    real_part = charge[0][:, None] * cheb_first - charge[1][:, None] * cheb_second
    imag_part = charge[0][:, None] * cheb_second + charge[1][:, None] * cheb_first
    return jnp.concatenate([real_part, imag_part], axis=1)


def merge_children(children, operators):
    row_count, col_count, coeff_width = children.shape
    grouped = children.reshape(row_count // 2, 2, col_count // 2, 2, coeff_width)
    parent = jnp.zeros(((row_count // 2) * (col_count // 2), coeff_width), jnp.float32)
    for row_bit in range(2):
        for col_bit in range(2):
            quarter = grouped[:, row_bit, :, col_bit, :].reshape(-1, coeff_width)
            parent = parent + jnp.dot(quarter, operators[2 * row_bit + col_bit], precision=HIGHEST, preferred_element_type=jnp.float32)
    return parent.reshape(row_count // 2, col_count // 2, coeff_width)


def transfer(padded, diagonal, row_start, col_start, row_count, col_count):
    half_width = diagonal.shape[1] // 2
    row_parity = (row_start + jnp.arange(row_count, dtype=jnp.int32)) % 2
    col_parity = (col_start + jnp.arange(col_count, dtype=jnp.int32)) % 2
    summed = jnp.zeros((row_count, col_count, diagonal.shape[1]), jnp.float32)
    for shift_row in range(-3, 4):
        for shift_col in range(-3, 4):
            if max(abs(shift_row), abs(shift_col)) < 2:
                continue
            row_ok = ((shift_row >= -2 - row_parity) & (shift_row <= 3 - row_parity)).astype(jnp.float32)
            col_ok = ((shift_col >= -2 - col_parity) & (shift_col <= 3 - col_parity)).astype(jnp.float32)
            allowed = row_ok[:, None] * col_ok[None, :]
            source = padded[3 + shift_row:3 + shift_row + row_count, 3 + shift_col:3 + shift_col + col_count, :]
            factor = diagonal[(shift_row + 3) * 7 + shift_col + 3]
            diag_real = factor[:half_width]
            diag_imag = factor[half_width:]
            src_real = source[..., :half_width]
            src_imag = source[..., half_width:]
            product = jnp.concatenate([diag_real * src_real - diag_imag * src_imag, diag_real * src_imag + diag_imag * src_real], axis=-1)
            summed = summed + allowed[:, :, None] * product
    return summed


def pad_grid(current):
    return jnp.pad(current, ((3, 3), (3, 3), (0, 0)))


def whole_transfer(current, diagonal):
    return transfer(pad_grid(current), diagonal, 0, 0, current.shape[0], current.shape[1])


def reference(offsets, strengths, leaf_map, shift_matrices, transfer_diagonal):
    grid_rows = N_WIDE * LEAF_SIDE
    grid_cols = N_NARROW * LEAF_SIDE
    wide_id = lax.broadcasted_iota(jnp.int32, leaf_map.shape, 0)
    narrow_id = lax.broadcasted_iota(jnp.int32, leaf_map.shape, 1)
    global_row = wide_id * LEAF_SIDE + leaf_map // LEAF_SIDE
    global_col = narrow_id * LEAF_SIDE + leaf_map % LEAF_SIDE
    segment = (global_row * grid_cols + global_col).reshape(-1).astype(jnp.int32)
    flat_coords = offsets.reshape(2, -1)
    flat_charge = strengths.reshape(2, -1)
    panel_total = flat_coords.shape[1]
    block_size = math.gcd(panel_total, 131072)
    block_count = panel_total // block_size

    def add_block(totals, number):
        begin = (number * block_size).astype(jnp.int32)
        coords = lax.dynamic_slice_in_dim(flat_coords, begin, block_size, 1)
        charge = lax.dynamic_slice_in_dim(flat_charge, begin, block_size, 1)
        pieces = lax.dynamic_slice_in_dim(segment, begin, block_size, 0)
        return totals + jax.ops.segment_sum(panel_terms(coords, charge), pieces, num_segments=grid_rows * grid_cols), None

    totals, _ = lax.scan(add_block, jnp.zeros((grid_rows * grid_cols, 2 * ORDER), jnp.float32), jnp.arange(block_count, dtype=jnp.int32))
    leaf_grid = totals.reshape(grid_rows, grid_cols, 2 * ORDER)
    levels = {LOCAL: leaf_grid}
    for level in range(LOCAL - 1, -1, -1):
        levels[level] = merge_children(levels[level + 1], shift_matrices[COARSE + level])
    coarse_grid = merge_children(levels[0], shift_matrices[1])
    top_grid = merge_children(coarse_grid, shift_matrices[0])
    coarse_local = whole_transfer(coarse_grid, transfer_diagonal[0])
    local_zero = whole_transfer(levels[0], transfer_diagonal[1])
    local_one = whole_transfer(levels[1], transfer_diagonal[2])
    local_two = whole_transfer(levels[2], transfer_diagonal[3])
    local_three = whole_transfer(levels[3], transfer_diagonal[4])
    return (leaf_grid, local_zero, local_one, local_two, local_three, coarse_local, top_grid)
```

```python
import functools

import jax
import jax.numpy as jnp
from jax import lax
from jax.experimental import pallas as pl
from jax.experimental.pallas import tpu as pltpu
from jax.sharding import PartitionSpec as P

F32 = jnp.float32
BF16 = jnp.bfloat16
MESH = pl.DeviceIdType.MESH
COARSE = 2
SIDE = 32
REACH = 3


def split(x):
    hi = x.astype(BF16)
    return hi, (x - hi.astype(F32)).astype(BF16)


def dot(a, b):
    return jnp.dot(a, b, preferred_element_type=F32)


def merge(parts, weight):
    width = parts[0].shape[1]
    lhs = jnp.concatenate(parts, axis=1)
    hi, lo = split(lhs)
    w_hi, w_lo = split(weight)
    both = dot(hi, jnp.concatenate([w_hi, w_lo], axis=1))
    return both[:, :width] + (both[:, width:] + dot(lo, w_hi))


def cheb_start(a):
    k = lax.broadcasted_iota(jnp.int32, a.shape, 0)
    t = [jnp.ones_like(a), a]
    twice = a + a
    for _ in range(7):
        t.append(twice * t[-1] - t[-2])
    cur, prev = t[0], t[8]
    for n in range(1, 8):
        cur = jnp.where(k == n, t[n], cur)
        prev = jnp.where(k == n, t[8 - n], prev)
    return t[8] + t[8], prev, cur


def panel_kernel(order, chunk, off_ref, str_ref, map_ref, shift_ref, leaf_ref, l3_ref, l2_ref, l01_ref, acc_ref):
    panels = off_ref.shape[-1]
    leaves = SIDE * SIDE
    acc_ref[...] = jnp.zeros_like(acc_ref)

    def body(i, carry):
        at = pl.ds(pl.multiple_of(i * chunk, chunk), chunk)
        wide8 = lambda ref, n: jnp.broadcast_to(ref[n, 0, :, at], (8, chunk))
        a, b = wide8(off_ref, 0), wide8(off_ref, 1)
        qr, qi = wide8(str_ref, 0), wide8(str_ref, 1)
        ma, pa, ca = cheb_start(a)
        mb, pb, cb = cheb_start(b)
        real, imag = [], []
        for j in range(order // 8):
            real.append(qr * ca - qi * cb)
            imag.append(qr * cb + qi * ca)
            if j + 1 < order // 8:
                ca, pa = ma * ca - pa, ca
                cb, pb = mb * cb - pb, cb
        hi, lo = split(jnp.concatenate(real + imag, axis=0))
        terms = jnp.concatenate([hi, lo], axis=0)
        leaf = jnp.broadcast_to(map_ref[0, :, at], (SIDE, chunk))
        row = (leaf // SIDE).astype(F32).astype(BF16)
        col = leaf % SIDE
        one = (col == lax.broadcasted_iota(jnp.int32, (SIDE, chunk), 0)).astype(F32).astype(BF16)
        zero = jnp.zeros_like(one)
        sel = jnp.concatenate([jnp.where(row == r, one, zero) for r in range(SIDE)], axis=0)
        acc_ref[...] += lax.dot_general(sel, terms, (((1,), (1,)), ((), ())), preferred_element_type=F32)
        return carry

    lax.fori_loop(0, panels // chunk, body, 0)
    width = 2 * order
    leaf_ref[...] = acc_ref[:, :width] + acc_ref[:, width:]

    def weight(level):
        return shift_ref[COARSE + level].reshape(4 * width, width)

    parts = []
    for r0 in range(2):
        for c0 in range(2):
            rows = []
            for r1 in range(2):
                for c1 in range(2):
                    for top in range(8):
                        start = (4 * top + 2 * r1 + r0) * SIDE + 2 * c1 + c0
                        rows.append(leaf_ref[pl.ds(start, 8, stride=4), :])
            parts.append(jnp.concatenate(rows, axis=0))
    level4 = merge(parts, weight(4))
    level3 = merge([level4[64 * q : 64 * q + 64] for q in range(4)], weight(3))
    l3_ref[...] = level3
    parts = []
    for rb in range(2):
        for cb in range(2):
            parts.append(jnp.concatenate([l3_ref[pl.ds((2 * r + rb) * 8 + cb, 4, stride=2), :] for r in range(4)], axis=0))
    l2_ref[...] = merge(parts, weight(2))
    parts = []
    for rb in range(2):
        for cb in range(2):
            parts.append(jnp.concatenate([l2_ref[pl.ds((2 * r + rb) * 4 + cb, 2, stride=2), :] for r in range(2)], axis=0))
    level1 = merge(parts, weight(1))
    level0 = merge([level1[q : q + 1] for q in range(4)], weight(0))
    l01_ref[...] = jnp.concatenate([level0, level1, jnp.zeros((3, width), F32)], axis=0)


NEAR = [(dr, dc) for dr in range(-3, 4) for dc in range(-3, 4) if max(abs(dr), abs(dc)) >= 2]
AROUND = [(dw, dv) for dw in (-1, 0, 1) for dv in (-1, 0, 1) if (dw, dv) != (0, 0)]


def allowed(d, parity):
    return -2 - parity <= d <= 3 - parity


def exchange_kernel(
    rows, cols,
    l3_ref, l2_ref, l01_ref, shift_ref, diag_ref,
    zero_out, one_out, two_out, three_out, coarse_out, top_out,
    reg3, slots2, big, pad2, sh3, sh2, xr, xi, lhs, grid1,
    send_all, recv_all, send_near, recv_near,
):
    w, v = lax.axis_index("wide"), lax.axis_index("narrow")
    count = rows * cols
    me = w * cols + v
    width = l01_ref.shape[-1]
    half = width // 2

    barrier = pltpu.get_barrier_semaphore()

    def greet(i, carry):
        t = lax.rem(me + i, count)
        pl.semaphore_signal(barrier, inc=1, device_id=(t // cols, lax.rem(t, cols)), device_id_type=MESH)
        return carry

    lax.fori_loop(1, count, greet, 0)
    pl.semaphore_wait(barrier, count - 1)

    row_of = {-1: 0, 0: 0, 1: 5}
    row_to = {-1: 11, 0: 3, 1: 0}
    row_n = {-1: 3, 0: 8, 1: 3}
    col_to = {-1: 16, 0: 8, 1: 0}

    def inside(dw, dv):
        ok = jnp.bool_(True)
        if dw < 0:
            ok = w > 0
        if dw > 0:
            ok = w < rows - 1
        if dv < 0:
            ok = ok & (v > 0)
        if dv > 0:
            ok = ok & (v < cols - 1)
        return ok

    def near_copies(dw, dv):
        slot = (1 - dw) * 3 + (1 - dv)
        target = (w + dw, v + dv)
        three = pltpu.make_async_remote_copy(
            src_ref=l3_ref.at[pl.ds(row_of[dw], row_n[dw])],
            dst_ref=reg3.at[pl.ds(row_to[dw], row_n[dw]), pl.ds(col_to[dv], 8)],
            send_sem=send_near.at[0, slot], recv_sem=recv_near.at[0, slot],
            device_id=target, device_id_type=MESH)
        two = pltpu.make_async_remote_copy(
            src_ref=l2_ref, dst_ref=slots2.at[slot],
            send_sem=send_near.at[1, slot], recv_sem=recv_near.at[1, slot],
            device_id=target, device_id_type=MESH)
        return three, two

    def all_copy(t, source):
        sw, sv = source // cols, lax.rem(source, cols)
        return pltpu.make_async_remote_copy(
            src_ref=l01_ref, dst_ref=big.at[3 + sw, 3 + sv],
            send_sem=send_all.at[t], recv_sem=recv_all.at[source],
            device_id=(t // cols, lax.rem(t, cols)), device_id_type=MESH)

    def send(i, carry):
        all_copy(lax.rem(me + i, count), me).start()
        return carry

    lax.fori_loop(1, count, send, 0)
    for dw, dv in AROUND:
        @pl.when(inside(dw, dv))
        def _():
            for copy in near_copies(dw, dv):
                copy.start()

    tile = jnp.zeros((8, width), F32)
    for dw, dv in AROUND:
        @pl.when(jnp.logical_not(inside(dw, dv)))
        def _():
            for r in range(row_n[-dw]):
                reg3[row_to[-dw] + r, pl.ds(col_to[-dv], 8)] = tile
            slot = (1 + dw) * 3 + (1 + dv)
            slots2[slot] = jnp.zeros((16, width), F32)
    for r in range(rows + 6):
        for c in range(cols + 6):
            if not (3 <= r < rows + 3 and 3 <= c < cols + 3):
                big[r, c] = tile
    big[3 + w, 3 + v] = l01_ref[...]
    for r in range(8):
        reg3[3 + r, pl.ds(8, 8)] = l3_ref[r]
    slots2[4] = l2_ref[...]
    for r in range(10):
        pad2[r, pl.ds(8, 8)] = tile

    lane = lax.broadcasted_iota(jnp.int32, (diag_ref.shape[1], width), 1) < half
    for s in range(diag_ref.shape[0]):
        d = diag_ref[s]
        turned = pltpu.roll(d, half, 1)
        xr[s] = jnp.where(lane, d, turned)
        xi[s] = jnp.where(lane, turned, d)
    sign = jnp.where(lax.broadcasted_iota(jnp.int32, (1, width), 1) < half, -1.0, 1.0).astype(F32)
    c_id = lax.broadcasted_iota(jnp.int32, (8, width), 0)
    odd = lax.rem(c_id, 2) == 1

    def col_mask(dc, slab):
        if dc == -3:
            return jnp.where(odd, slab, 0.0)
        if dc == 3:
            return jnp.where(odd, 0.0, slab)
        return slab

    def factor(s, dr, dc):
        at = pl.ds(7 * (dr + 3) + dc + 3, 1)
        return xr[s, at, :], xi[s, at, :]

    def finish(acc_r, acc_i):
        return acc_r + sign * pltpu.roll(acc_i, half, 1)

    def near_level(s, n, shifted, out):
        acc_r = [jnp.zeros((8, width), F32) for _ in range(n)]
        acc_i = [jnp.zeros((8, width), F32) for _ in range(n)]
        for dr, dc in NEAR:
            f_r, f_i = factor(s, dr, dc)
            for r in range(n):
                if allowed(dr, r % 2):
                    src = shifted[dc + 3, 3 + r + dr]
                    acc_r[r] = acc_r[r] + f_r * src
                    acc_i[r] = acc_i[r] + f_i * src
        for r in range(n):
            out[r] = finish(acc_r[r], acc_i[r])[: out.shape[1]]

    for dw, dv in AROUND:
        @pl.when(inside(dw, dv))
        def _():
            for copy in near_copies(-dw, -dv):
                copy.wait_recv()

    for dc in range(-3, 4):
        for r in range(14):
            sh3[dc + 3, r] = col_mask(dc, reg3[r, pl.ds(8 + dc, 8)])
    near_level(4, 8, sh3, three_out)

    for dw in (-1, 0, 1):
        for dv in (-1, 0, 1):
            slot = (1 + dw) * 3 + (1 + dv)
            for r in range(4):
                at = 3 + 4 * dw + r
                if 0 <= at < 10:
                    pad2[at, pl.ds(4 + 4 * dv, 4)] = slots2[slot, pl.ds(4 * r, 4)]
    for dc in range(-3, 4):
        for r in range(10):
            sh2[dc + 3, r] = col_mask(dc, pad2[r, pl.ds(4 + dc, 8)])
    near_level(3, 4, sh2, two_out)

    def arrive(i, carry):
        s = lax.rem(me + i, count)
        all_copy(s, s).wait_recv()
        return carry

    lax.fori_loop(1, count, arrive, 0)

    half_r, half_c = rows // 2, cols // 2
    for r in range(rows):
        for c in range(cols):
            q = 2 * (r % 2) + c % 2
            lhs[pl.ds((r // 2) * half_c + c // 2, 1), pl.ds(q * width, width)] = big[3 + r, 3 + c, pl.ds(0, 1)]
    boxes = half_r * half_c

    def weight(t):
        return shift_ref[t].reshape(4 * width, width)

    coarse = merge([lhs[:boxes, pl.ds(q * width, width)] for q in range(4)], weight(1))
    grid1[:boxes] = coarse
    quarter_c = half_c // 2
    for r in range(half_r):
        for c in range(half_c):
            q = 2 * (r % 2) + c % 2
            lhs[pl.ds((r // 2) * quarter_c + c // 2, 1), pl.ds(q * width, width)] = grid1[pl.ds(r * half_c + c, 1)]
    tops = (half_r // 2) * quarter_c
    top = merge([lhs[:tops, pl.ds(q * width, width)] for q in range(4)], weight(0))
    for r in range(half_r // 2):
        top_out[r] = top[r * quarter_c : (r + 1) * quarter_c]

    for tr in range(2):
        line = []
        for tc in range(2):
            acc_r = jnp.zeros((1, width), F32)
            acc_i = jnp.zeros((1, width), F32)
            for dr, dc in NEAR:
                if allowed(dr, tr) and allowed(dc, tc):
                    f_r, f_i = factor(2, dr, dc)
                    sr, sc = tr + dr, tc + dc
                    src = big[3 + w + sr // 2, 3 + v + sc // 2, pl.ds(1 + 2 * (sr % 2) + sc % 2, 1)]
                    acc_r = acc_r + f_r * src
                    acc_i = acc_i + f_i * src
            line.append(finish(acc_r, acc_i))
        one_out[tr] = jnp.concatenate(line, axis=0)

    odd_w, odd_v = lax.rem(w, 2), lax.rem(v, 2)
    keep = {
        ("r", -3): odd_w.astype(F32), ("r", 3): (1 - odd_w).astype(F32),
        ("c", -3): odd_v.astype(F32), ("c", 3): (1 - odd_v).astype(F32),
    }
    acc_r = jnp.zeros((1, width), F32)
    acc_i = jnp.zeros((1, width), F32)
    for dr, dc in NEAR:
        f_r, f_i = factor(1, dr, dc)
        src = big[3 + w + dr, 3 + v + dc, pl.ds(0, 1)]
        if abs(dr) == 3:
            src = src * keep["r", dr]
        if abs(dc) == 3:
            src = src * keep["c", dc]
        acc_r = acc_r + f_r * src
        acc_i = acc_i + f_i * src
    zero_out[0] = finish(acc_r, acc_i)

    for r in range(half_r):
        line = []
        for c in range(half_c):
            acc_r = jnp.zeros((1, width), F32)
            acc_i = jnp.zeros((1, width), F32)
            for dr, dc in NEAR:
                if allowed(dr, r % 2) and allowed(dc, c % 2) and 0 <= r + dr < half_r and 0 <= c + dc < half_c:
                    f_r, f_i = factor(0, dr, dc)
                    src = grid1[pl.ds((r + dr) * half_c + c + dc, 1)]
                    acc_r = acc_r + f_r * src
                    acc_i = acc_i + f_i * src
            line.append(finish(acc_r, acc_i))
        coarse_out[r] = jnp.concatenate(line, axis=0)

    for dw, dv in AROUND:
        @pl.when(inside(dw, dv))
        def _():
            for copy in near_copies(dw, dv):
                copy.wait_send()

    def left(i, carry):
        all_copy(lax.rem(me + i, count), me).wait_send()
        return carry

    lax.fori_loop(1, count, left, 0)


def local(mesh_shape, offsets, strengths, leaf_map, shift_matrices, transfer_diagonal):
    rows, cols = mesh_shape
    width = shift_matrices.shape[-1]
    order = width // 2
    levels = transfer_diagonal.shape[0]
    vmem = pl.BlockSpec(memory_space=pltpu.VMEM)
    shape = lambda *dims: jax.ShapeDtypeStruct(dims, F32)
    leaf, l3, l2, l01 = pl.pallas_call(
        functools.partial(panel_kernel, order, 512),
        out_shape=(shape(SIDE * SIDE, width), shape(64, width), shape(16, width), shape(8, width)),
        in_specs=[vmem] * 4,
        out_specs=(vmem,) * 4,
        scratch_shapes=[pltpu.VMEM((SIDE * SIDE, 2 * width), F32)],
        name="panels",
    )(offsets, strengths, leaf_map, shift_matrices)
    boxes = (rows // 2) * (cols // 2)
    pad8 = -(-boxes // 8) * 8
    outs = pl.pallas_call(
        functools.partial(exchange_kernel, rows, cols),
        out_shape=(
            shape(1, 1, width), shape(2, 2, width), shape(4, 4, width), shape(8, 8, width),
            shape(rows // 2, cols // 2, width), shape(rows // 4, cols // 4, width),
        ),
        grid=(1,),
        in_specs=[vmem, vmem, vmem, pl.BlockSpec((2, 4, width, width), lambda i: (0, 0, 0, 0)), vmem],
        out_specs=(vmem,) * 6,
        scratch_shapes=[
            pltpu.VMEM((14, 24, width), F32),
            pltpu.VMEM((9, 16, width), F32),
            pltpu.VMEM((rows + 6, cols + 6, 8, width), F32),
            pltpu.VMEM((10, 16, width), F32),
            pltpu.VMEM((7, 14, 8, width), F32),
            pltpu.VMEM((7, 10, 8, width), F32),
            pltpu.VMEM((levels, 49, width), F32),
            pltpu.VMEM((levels, 49, width), F32),
            pltpu.VMEM((pad8, 4 * width), F32),
            pltpu.VMEM((pad8, width), F32),
            pltpu.SemaphoreType.DMA((rows * cols,)),
            pltpu.SemaphoreType.DMA((rows * cols,)),
            pltpu.SemaphoreType.DMA((2, 9)),
            pltpu.SemaphoreType.DMA((2, 9)),
        ],
        compiler_params=pltpu.CompilerParams(collective_id=0, has_side_effects=True),
        name="exchange",
    )(l3.reshape(8, 8, width), l2, l01, shift_matrices, transfer_diagonal)
    return (leaf.reshape(SIDE, SIDE, width),) + tuple(outs)


def solution(mesh):
    split_2 = P("wide", "narrow", None)
    in_specs = (P(None, "wide", "narrow", None), P(None, "wide", "narrow", None), split_2, P(), P())
    out_specs = (split_2,) * 5 + (P(), P())
    body = functools.partial(local, (mesh.shape["wide"], mesh.shape["narrow"]))
    return jax.shard_map(body, mesh=mesh, in_specs=in_specs, out_specs=out_specs, check_vma=False)
```

```python
import functools
import math

import jax
import jax.numpy as jnp
from jax import lax
from jax.experimental import pallas as pl
from jax.experimental.pallas import tpu as pltpu
from jax.sharding import PartitionSpec as P

F32 = jnp.float32
BF16 = jnp.bfloat16
MESH = pl.DeviceIdType.MESH
COARSE = 2
SIDE = 32
CHUNK = 2048
REACH = 3


def split(x):
    hi = x.astype(BF16)
    return hi, (x - hi.astype(F32)).astype(BF16)


def dot(a, b):
    return jnp.dot(a, b, preferred_element_type=F32)


def merge(parts, weight):
    width = parts[0].shape[1]
    lhs = jnp.concatenate(parts, axis=1)
    hi, lo = split(lhs)
    w_hi, w_lo = split(weight)
    both = dot(hi, jnp.concatenate([w_hi, w_lo], axis=1))
    return both[:, :width] + (both[:, width:] + dot(lo, w_hi))


def cheb_start(a):
    k = lax.broadcasted_iota(jnp.int32, a.shape, 0)
    t = [jnp.ones_like(a), a]
    twice = a + a
    for _ in range(7):
        t.append(twice * t[-1] - t[-2])
    cur, prev = t[0], t[8]
    for n in range(1, 8):
        cur = jnp.where(k == n, t[n], cur)
        prev = jnp.where(k == n, t[8 - n], prev)
    return t[8] + t[8], prev, cur


def panel_sums(order, chunk, off_ref, str_ref, map_ref, leaf_ref, acc_ref):
    panels = off_ref.shape[-1]
    acc_ref[...] = jnp.zeros_like(acc_ref)

    def body(i, carry):
        at = pl.ds(pl.multiple_of(i * chunk, chunk), chunk)
        wide8 = lambda ref, n: jnp.broadcast_to(ref[n, 0, :, at], (8, chunk))
        a, b = wide8(off_ref, 0), wide8(off_ref, 1)
        qr, qi = wide8(str_ref, 0), wide8(str_ref, 1)
        ma, pa, ca = cheb_start(a)
        mb, pb, cb = cheb_start(b)
        real, imag = [], []
        for j in range(order // 8):
            real.append(qr * ca - qi * cb)
            imag.append(qr * cb + qi * ca)
            if j + 1 < order // 8:
                ca, pa = ma * ca - pa, ca
                cb, pb = mb * cb - pb, cb
        hi, lo = split(jnp.concatenate(real + imag, axis=0))
        terms = jnp.concatenate([hi, lo], axis=0)
        leaf = jnp.broadcast_to(map_ref[0, :, at], (SIDE, chunk))
        row = (leaf // SIDE).astype(F32).astype(BF16)
        col = leaf % SIDE
        one = (col == lax.broadcasted_iota(jnp.int32, (SIDE, chunk), 0)).astype(F32).astype(BF16)
        zero = jnp.zeros_like(one)
        sel = jnp.concatenate([jnp.where(row == r, one, zero) for r in range(SIDE)], axis=0)
        acc_ref[...] += lax.dot_general(sel, terms, (((1,), (1,)), ((), ())), preferred_element_type=F32)
        return carry

    lax.fori_loop(0, panels // chunk, body, 0)
    width = 2 * order
    leaf_ref[...] = acc_ref[:, :width] + acc_ref[:, width:]


def upward(shift_ref, leaf_ref, l3_ref, l2_ref):
    width = leaf_ref.shape[-1]

    def weight(level):
        return shift_ref[COARSE + level].reshape(4 * width, width)

    parts = []
    for r0 in range(2):
        for c0 in range(2):
            rows = []
            for r1 in range(2):
                for c1 in range(2):
                    for top in range(8):
                        start = (4 * top + 2 * r1 + r0) * SIDE + 2 * c1 + c0
                        rows.append(leaf_ref[pl.ds(start, 8, stride=4), :])
            parts.append(jnp.concatenate(rows, axis=0))
    level4 = merge(parts, weight(4))
    level3 = merge([level4[64 * q : 64 * q + 64] for q in range(4)], weight(3))
    l3_ref[...] = level3
    parts = []
    for rb in range(2):
        for cb in range(2):
            parts.append(jnp.concatenate([l3_ref[pl.ds((2 * r + rb) * 8 + cb, 4, stride=2), :] for r in range(4)], axis=0))
    l2_ref[...] = merge(parts, weight(2))
    parts = []
    for rb in range(2):
        for cb in range(2):
            parts.append(jnp.concatenate([l2_ref[pl.ds((2 * r + rb) * 4 + cb, 2, stride=2), :] for r in range(2)], axis=0))
    level1 = merge(parts, weight(1))
    level0 = merge([level1[q : q + 1] for q in range(4)], weight(0))
    return jnp.concatenate([level0, level1, jnp.zeros((3, width), F32)], axis=0)


NEAR = [(dr, dc) for dr in range(-3, 4) for dc in range(-3, 4) if max(abs(dr), abs(dc)) >= 2]
AROUND = [(dw, dv) for dw in (-1, 0, 1) for dv in (-1, 0, 1) if (dw, dv) != (0, 0)]


def allowed(d, parity):
    return -2 - parity <= d <= 3 - parity


def tree_kernel(
    rows, cols, chunk,
    off_ref, str_ref, map_ref, shift_in, diag_in,
    leaf_ref, zero_out, one_out, two_out, three_out, coarse_out, top_out,
    acc_ref, shift_ref, diag_ref, l3_flat, l3_ref, l2_ref, l01_ref, load_sem, reg3, slots2, big, pad2, sh3, sh2, xr, xi, lhs, grid1,
    send_all, recv_all, send_near, recv_near,
):
    w, v = lax.axis_index("wide"), lax.axis_index("narrow")
    count = rows * cols
    width = diag_ref.shape[-1]
    half = width // 2

    to_w = [lax.rem(w + i, rows) for i in range(rows)]
    to_v = [lax.rem(v + j, cols) for j in range(cols)]
    from_w = [lax.rem(w + rows - i, rows) for i in range(rows)]
    from_v = [lax.rem(v + cols - j, cols) for j in range(cols)]
    others = [(i, j) for i in range(rows) for j in range(cols) if (i, j) != (0, 0)]

    barrier = pltpu.get_barrier_semaphore()
    for i, j in others:
        pl.semaphore_signal(barrier, inc=1, device_id=(to_w[i], to_v[j]), device_id_type=MESH)
    loads = [
        pltpu.make_async_copy(shift_in, shift_ref, load_sem.at[0]),
        pltpu.make_async_copy(diag_in, diag_ref, load_sem.at[1]),
    ]
    for load in loads:
        load.start()

    panel_sums(half, chunk, off_ref, str_ref, map_ref, leaf_ref, acc_ref)
    for load in loads:
        load.wait()
    l01_ref[...] = upward(shift_ref, leaf_ref, l3_flat, l2_ref)
    for r in range(8):
        block = l3_flat[pl.ds(8 * r, 8)]
        l3_ref[r] = block
        reg3[3 + r, pl.ds(8, 8)] = block
    slots2[4] = l2_ref[...]
    big[3 + w, 3 + v] = l01_ref[...]
    pl.semaphore_wait(barrier, count - 1)

    row_of = {-1: 0, 0: 0, 1: 5}
    row_to = {-1: 11, 0: 3, 1: 0}
    row_n = {-1: 3, 0: 8, 1: 3}
    col_to = {-1: 16, 0: 8, 1: 0}

    def inside(dw, dv):
        ok = jnp.bool_(True)
        if dw < 0:
            ok = w > 0
        if dw > 0:
            ok = w < rows - 1
        if dv < 0:
            ok = ok & (v > 0)
        if dv > 0:
            ok = ok & (v < cols - 1)
        return ok

    def near_copies(dw, dv):
        slot = (1 - dw) * 3 + (1 - dv)
        target = (w + dw, v + dv)
        three = pltpu.make_async_remote_copy(
            src_ref=l3_ref.at[pl.ds(row_of[dw], row_n[dw])],
            dst_ref=reg3.at[pl.ds(row_to[dw], row_n[dw]), pl.ds(col_to[dv], 8)],
            send_sem=send_near.at[0, slot], recv_sem=recv_near.at[0, slot],
            device_id=target, device_id_type=MESH)
        two = pltpu.make_async_remote_copy(
            src_ref=l2_ref, dst_ref=slots2.at[slot],
            send_sem=send_near.at[1, slot], recv_sem=recv_near.at[1, slot],
            device_id=target, device_id_type=MESH)
        return three, two

    def all_copy(i, j, source):
        return pltpu.make_async_remote_copy(
            src_ref=l01_ref, dst_ref=big.at[3 + source[0], 3 + source[1]],
            send_sem=send_all.at[i * cols + j], recv_sem=recv_all.at[i * cols + j],
            device_id=(to_w[i], to_v[j]), device_id_type=MESH)

    for i, j in others:
        all_copy(i, j, (w, v)).start()
    for dw, dv in AROUND:
        @pl.when(inside(dw, dv))
        def _():
            for copy in near_copies(dw, dv):
                copy.start()

    tile = jnp.zeros((8, width), F32)
    for dw, dv in AROUND:
        @pl.when(jnp.logical_not(inside(dw, dv)))
        def _():
            for r in range(row_n[-dw]):
                reg3[row_to[-dw] + r, pl.ds(col_to[-dv], 8)] = tile
            slot = (1 + dw) * 3 + (1 + dv)
            slots2[slot] = jnp.zeros((16, width), F32)
    for r in range(rows + 6):
        for c in range(cols + 6):
            if not (3 <= r < rows + 3 and 3 <= c < cols + 3):
                big[r, c] = tile
    for r in range(10):
        pad2[r, pl.ds(8, 8)] = tile

    lane = lax.broadcasted_iota(jnp.int32, (diag_ref.shape[1], width), 1) < half
    for s in range(diag_ref.shape[0]):
        d = diag_ref[s]
        turned = pltpu.roll(d, half, 1)
        xr[s] = jnp.where(lane, d, turned)
        xi[s] = jnp.where(lane, turned, d)
    sign = jnp.where(lax.broadcasted_iota(jnp.int32, (1, width), 1) < half, -1.0, 1.0).astype(F32)
    c_id = lax.broadcasted_iota(jnp.int32, (8, width), 0)
    odd = lax.rem(c_id, 2) == 1

    def col_mask(dc, slab):
        if dc == -3:
            return jnp.where(odd, slab, 0.0)
        if dc == 3:
            return jnp.where(odd, 0.0, slab)
        return slab

    def factor(s, dr, dc):
        at = pl.ds(7 * (dr + 3) + dc + 3, 1)
        return xr[s, at, :], xi[s, at, :]

    def finish(acc_r, acc_i):
        return acc_r + sign * pltpu.roll(acc_i, half, 1)

    def near_level(s, n, shifted, out):
        acc_r = [jnp.zeros((8, width), F32) for _ in range(n)]
        acc_i = [jnp.zeros((8, width), F32) for _ in range(n)]
        for dr, dc in NEAR:
            f_r, f_i = factor(s, dr, dc)
            for r in range(n):
                if allowed(dr, r % 2):
                    src = shifted[dc + 3, 3 + r + dr]
                    acc_r[r] = acc_r[r] + f_r * src
                    acc_i[r] = acc_i[r] + f_i * src
        for r in range(n):
            out[r] = finish(acc_r[r], acc_i[r])[: out.shape[1]]

    for dw, dv in AROUND:
        @pl.when(inside(dw, dv))
        def _():
            for copy in near_copies(-dw, -dv):
                copy.wait_recv()

    for dc in range(-3, 4):
        for r in range(14):
            sh3[dc + 3, r] = col_mask(dc, reg3[r, pl.ds(8 + dc, 8)])
    near_level(4, 8, sh3, three_out)

    for dw in (-1, 0, 1):
        for dv in (-1, 0, 1):
            slot = (1 + dw) * 3 + (1 + dv)
            for r in range(4):
                at = 3 + 4 * dw + r
                if 0 <= at < 10:
                    pad2[at, pl.ds(4 + 4 * dv, 4)] = slots2[slot, pl.ds(4 * r, 4)]
    for dc in range(-3, 4):
        for r in range(10):
            sh2[dc + 3, r] = col_mask(dc, pad2[r, pl.ds(4 + dc, 8)])
    near_level(3, 4, sh2, two_out)

    for i, j in others:
        all_copy(i, j, (from_w[i], from_v[j])).wait_recv()

    half_r, half_c = rows // 2, cols // 2
    for r in range(rows):
        for c in range(cols):
            q = 2 * (r % 2) + c % 2
            lhs[pl.ds((r // 2) * half_c + c // 2, 1), pl.ds(q * width, width)] = big[3 + r, 3 + c, pl.ds(0, 1)]
    boxes = half_r * half_c

    def weight(t):
        return shift_ref[t].reshape(4 * width, width)

    coarse = merge([lhs[:boxes, pl.ds(q * width, width)] for q in range(4)], weight(1))
    grid1[:boxes] = coarse
    quarter_c = half_c // 2
    for r in range(half_r):
        for c in range(half_c):
            q = 2 * (r % 2) + c % 2
            lhs[pl.ds((r // 2) * quarter_c + c // 2, 1), pl.ds(q * width, width)] = grid1[pl.ds(r * half_c + c, 1)]
    tops = (half_r // 2) * quarter_c
    top = merge([lhs[:tops, pl.ds(q * width, width)] for q in range(4)], weight(0))
    for r in range(half_r // 2):
        top_out[r] = top[r * quarter_c : (r + 1) * quarter_c]

    for tr in range(2):
        line = []
        for tc in range(2):
            acc_r = jnp.zeros((1, width), F32)
            acc_i = jnp.zeros((1, width), F32)
            for dr, dc in NEAR:
                if allowed(dr, tr) and allowed(dc, tc):
                    f_r, f_i = factor(2, dr, dc)
                    sr, sc = tr + dr, tc + dc
                    src = big[3 + w + sr // 2, 3 + v + sc // 2, pl.ds(1 + 2 * (sr % 2) + sc % 2, 1)]
                    acc_r = acc_r + f_r * src
                    acc_i = acc_i + f_i * src
            line.append(finish(acc_r, acc_i))
        one_out[tr] = jnp.concatenate(line, axis=0)

    odd_w, odd_v = lax.rem(w, 2), lax.rem(v, 2)
    keep = {
        ("r", -3): odd_w.astype(F32), ("r", 3): (1 - odd_w).astype(F32),
        ("c", -3): odd_v.astype(F32), ("c", 3): (1 - odd_v).astype(F32),
    }
    acc_r = jnp.zeros((1, width), F32)
    acc_i = jnp.zeros((1, width), F32)
    for dr, dc in NEAR:
        f_r, f_i = factor(1, dr, dc)
        src = big[3 + w + dr, 3 + v + dc, pl.ds(0, 1)]
        if abs(dr) == 3:
            src = src * keep["r", dr]
        if abs(dc) == 3:
            src = src * keep["c", dc]
        acc_r = acc_r + f_r * src
        acc_i = acc_i + f_i * src
    zero_out[0] = finish(acc_r, acc_i)

    for r in range(half_r):
        line = []
        for c in range(half_c):
            acc_r = jnp.zeros((1, width), F32)
            acc_i = jnp.zeros((1, width), F32)
            for dr, dc in NEAR:
                if allowed(dr, r % 2) and allowed(dc, c % 2) and 0 <= r + dr < half_r and 0 <= c + dc < half_c:
                    f_r, f_i = factor(0, dr, dc)
                    src = grid1[pl.ds((r + dr) * half_c + c + dc, 1)]
                    acc_r = acc_r + f_r * src
                    acc_i = acc_i + f_i * src
            line.append(finish(acc_r, acc_i))
        coarse_out[r] = jnp.concatenate(line, axis=0)

    for dw, dv in AROUND:
        @pl.when(inside(dw, dv))
        def _():
            for copy in near_copies(dw, dv):
                copy.wait_send()

    for i, j in others:
        all_copy(i, j, (w, v)).wait_send()


def write_kernel(n, *refs):
    sem = refs[2 * n]
    copies = [pltpu.make_async_copy(refs[k], refs[n + k], sem.at[k]) for k in range(n)]
    for copy in copies:
        copy.start()
    for copy in copies:
        copy.wait()


def local(mesh_shape, offsets, strengths, leaf_map, shift_matrices, transfer_diagonal):
    rows, cols = mesh_shape
    width = shift_matrices.shape[-1]
    levels = transfer_diagonal.shape[0]
    vmem = pl.BlockSpec(memory_space=pltpu.VMEM)
    boxes = (rows // 2) * (cols // 2)
    pad8 = -(-boxes // 8) * 8
    dims = (
        (SIDE * SIDE, width), (1, 1, width), (2, 2, width), (4, 4, width), (8, 8, width),
        (rows // 2, cols // 2, width), (rows // 4, cols // 4, width),
    )
    any_space = pl.BlockSpec(memory_space=pl.ANY)
    held = pl.pallas_call(
        functools.partial(tree_kernel, rows, cols, math.gcd(CHUNK, offsets.shape[-1])),
        out_shape=tuple(pltpu.VMEM(d, F32) for d in dims),
        in_specs=[vmem, vmem, vmem, any_space, any_space],
        out_specs=(vmem,) * len(dims),
        scratch_shapes=[
            pltpu.VMEM((SIDE * SIDE, 2 * width), F32),
            pltpu.VMEM(shift_matrices.shape, F32),
            pltpu.VMEM(transfer_diagonal.shape, F32),
            pltpu.VMEM((64, width), F32),
            pltpu.VMEM((8, 8, width), F32),
            pltpu.VMEM((16, width), F32),
            pltpu.VMEM((8, width), F32),
            pltpu.SemaphoreType.DMA((2,)),
            pltpu.VMEM((14, 24, width), F32),
            pltpu.VMEM((9, 16, width), F32),
            pltpu.VMEM((rows + 6, cols + 6, 8, width), F32),
            pltpu.VMEM((10, 16, width), F32),
            pltpu.VMEM((7, 14, 8, width), F32),
            pltpu.VMEM((7, 10, 8, width), F32),
            pltpu.VMEM((levels, 49, width), F32),
            pltpu.VMEM((levels, 49, width), F32),
            pltpu.VMEM((pad8, 4 * width), F32),
            pltpu.VMEM((pad8, width), F32),
            pltpu.SemaphoreType.DMA((rows * cols,)),
            pltpu.SemaphoreType.DMA((rows * cols,)),
            pltpu.SemaphoreType.DMA((2, 9)),
            pltpu.SemaphoreType.DMA((2, 9)),
        ],
        compiler_params=pltpu.CompilerParams(collective_id=0, has_side_effects=True),
        name="tree",
    )(offsets, strengths, leaf_map, shift_matrices, transfer_diagonal)
    n = len(dims)
    outs = pl.pallas_call(
        functools.partial(write_kernel, n),
        out_shape=tuple(jax.ShapeDtypeStruct(d, F32) for d in dims),
        in_specs=[vmem] * n,
        out_specs=(any_space,) * n,
        scratch_shapes=[pltpu.SemaphoreType.DMA((n,))],
        name="write",
    )(*[pltpu.with_memory_space_constraint(x, pltpu.VMEM) for x in held])
    return (outs[0].reshape(SIDE, SIDE, width),) + tuple(outs[1:])


def solution(mesh):
    split_2 = P("wide", "narrow", None)
    in_specs = (P(None, "wide", "narrow", None), P(None, "wide", "narrow", None), split_2, P(), P())
    out_specs = (split_2,) * 5 + (P(), P())
    body = functools.partial(local, (mesh.shape["wide"], mesh.shape["narrow"]))
    return jax.shard_map(body, mesh=mesh, in_specs=in_specs, out_specs=out_specs, check_vma=False)
```

```python
import functools
import math

import jax
import jax.numpy as jnp
from jax import lax
from jax.experimental import pallas as pl
from jax.experimental.pallas import tpu as pltpu
from jax.sharding import PartitionSpec as P

F32 = jnp.float32
BF16 = jnp.bfloat16
MESH = pl.DeviceIdType.MESH
COARSE = 2
SIDE = 32
CHUNK = 2048


def split(x):
    hi = x.astype(BF16)
    return hi, (x - hi.astype(F32)).astype(BF16)


def dot(a, b):
    return jnp.dot(a, b, preferred_element_type=F32)


def halves(weight):
    return jnp.concatenate(split(weight), axis=1)


def merge(parts, weight):
    width = parts[0].shape[1]
    lhs = jnp.concatenate(parts, axis=1)
    hi, lo = split(lhs)
    both = dot(hi, weight)
    return both[:, :width] + (both[:, width:] + dot(lo, weight[:, :width]))


def cheb_start(a):
    k = lax.broadcasted_iota(jnp.int32, a.shape, 0)
    t = [jnp.ones_like(a), a]
    twice = a + a
    for _ in range(7):
        t.append(twice * t[-1] - t[-2])
    cur, prev = t[0], t[8]
    for n in range(1, 8):
        cur = jnp.where(k == n, t[n], cur)
        prev = jnp.where(k == n, t[8 - n], prev)
    return t[8] + t[8], prev, cur


def panel_sums(order, chunk, off_ref, str_ref, map_ref, leaf_ref, acc_ref):
    panels = off_ref.shape[-1]

    def add(i, first):
        at = pl.ds(pl.multiple_of(i * chunk, chunk), chunk)
        wide8 = lambda ref, n: jnp.broadcast_to(ref[n, 0, :, at], (8, chunk))
        a, b = wide8(off_ref, 0), wide8(off_ref, 1)
        qr, qi = wide8(str_ref, 0), wide8(str_ref, 1)
        ma, pa, ca = cheb_start(a)
        mb, pb, cb = cheb_start(b)
        real, imag = [], []
        for j in range(order // 8):
            real.append(qr * ca - qi * cb)
            imag.append(qr * cb + qi * ca)
            if j + 1 < order // 8:
                ca, pa = ma * ca - pa, ca
                cb, pb = mb * cb - pb, cb
        hi, lo = split(jnp.concatenate(real + imag, axis=0))
        terms = jnp.concatenate([hi, lo], axis=0)
        leaf = jnp.broadcast_to(map_ref[0, :, at], (SIDE, chunk))
        row = (leaf // SIDE).astype(F32).astype(BF16)
        col = leaf % SIDE
        one = (col == lax.broadcasted_iota(jnp.int32, (SIDE, chunk), 0)).astype(F32).astype(BF16)
        zero = jnp.zeros_like(one)
        sel = jnp.concatenate([jnp.where(row == r, one, zero) for r in range(SIDE)], axis=0)
        part = lax.dot_general(sel, terms, (((1,), (1,)), ((), ())), preferred_element_type=F32)
        acc_ref[...] = part if first else acc_ref[...] + part

    def body(i, carry):
        add(i, False)
        return carry

    add(0, True)
    lax.fori_loop(1, panels // chunk, body, 0)
    width = 2 * order
    leaf_ref[...] = acc_ref[:, :width] + acc_ref[:, width:]


def upward(shift_ref, leaf_ref, l3_ref, l2_ref):
    width = leaf_ref.shape[-1]

    def weight(level):
        return halves(shift_ref[COARSE + level].reshape(4 * width, width))

    parts = []
    for r0 in range(2):
        for c0 in range(2):
            rows = []
            for r1 in range(2):
                for c1 in range(2):
                    for top in range(8):
                        start = (4 * top + 2 * r1 + r0) * SIDE + 2 * c1 + c0
                        rows.append(leaf_ref[pl.ds(start, 8, stride=4), :])
            parts.append(jnp.concatenate(rows, axis=0))
    level4 = merge(parts, weight(4))
    level3 = merge([level4[64 * q : 64 * q + 64] for q in range(4)], weight(3))
    l3_ref[...] = level3
    parts = []
    for rb in range(2):
        for cb in range(2):
            parts.append(jnp.concatenate([l3_ref[pl.ds((2 * r + rb) * 8 + cb, 4, stride=2), :] for r in range(4)], axis=0))
    l2_ref[...] = merge(parts, weight(2))
    parts = []
    for rb in range(2):
        for cb in range(2):
            parts.append(jnp.concatenate([l2_ref[pl.ds((2 * r + rb) * 4 + cb, 2, stride=2), :] for r in range(2)], axis=0))
    level1 = merge(parts, weight(1))
    level0 = merge([level1[q : q + 1] for q in range(4)], weight(0))
    return level1, level0


NEAR = [(dr, dc) for dr in range(-3, 4) for dc in range(-3, 4) if max(abs(dr), abs(dc)) >= 2]
AROUND = [(dw, dv) for dw in (-1, 0, 1) for dv in (-1, 0, 1) if (dw, dv) != (0, 0)]


def allowed(d, parity):
    return -2 - parity <= d <= 3 - parity


def tree_kernel(
    rows, cols, chunk,
    off_ref, str_ref, map_ref, shift_in, diag_in,
    leaf_ref, zero_out, one_out, two_out, three_out, coarse_out, top_out,
    acc_ref, shift_ref, diag_ref, l3_ref, l2_ref, l1_ref, l0_ref, load_sem,
    packed, landed, big, win3, win2, win1, sh3, sh2, sh1, xr, xi, lhs, grid1, coarse_w,
    send_all, recv_all, send_near, recv_near,
):
    w, v = lax.axis_index("wide"), lax.axis_index("narrow")
    count = rows * cols
    width = diag_ref.shape[-1]
    half = width // 2

    to_w = [lax.rem(w + i, rows) for i in range(rows)]
    to_v = [lax.rem(v + j, cols) for j in range(cols)]
    from_w = [lax.rem(w + rows - i, rows) for i in range(rows)]
    from_v = [lax.rem(v + cols - j, cols) for j in range(cols)]
    others = [(i, j) for i in range(rows) for j in range(cols) if (i, j) != (0, 0)]

    barrier = pltpu.get_barrier_semaphore()
    for i, j in others:
        pl.semaphore_signal(barrier, inc=1, device_id=(to_w[i], to_v[j]), device_id_type=MESH)
    loads = [
        pltpu.make_async_copy(shift_in, shift_ref, load_sem.at[0]),
        pltpu.make_async_copy(diag_in, diag_ref, load_sem.at[1]),
    ]
    for load in loads:
        load.start()

    panel_sums(half, chunk, off_ref, str_ref, map_ref, leaf_ref, acc_ref)
    for load in loads:
        load.wait()
    level1, level0 = upward(shift_ref, leaf_ref, l3_ref, l2_ref)
    l0_ref[...] = level0
    l1_ref[...] = jnp.concatenate([level1, jnp.zeros((4, width), F32)], axis=0)

    edge = {-1: 0, 1: 1}
    for dw, dv in AROUND:
        at = (1 + dw) * 3 + 1 + dv
        one_at = 24 if 0 in (dw, dv) else 8
        packed[at, pl.ds(one_at, 8)] = l1_ref[...]
        if dv == 0:
            packed[at, pl.ds(0, 16)] = l3_ref[pl.ds(48 * edge[dw], 16)]
            packed[at, pl.ds(16, 8)] = l2_ref[pl.ds(8 * edge[dw], 8)]
        elif dw == 0:
            for k in range(2):
                packed[at, pl.ds(8 * k, 8)] = l3_ref[pl.ds(6 * edge[dv] + k, 8, stride=8)]
                packed[at, pl.ds(16 + 4 * k, 4)] = l2_ref[pl.ds(2 * edge[dv] + k, 4, stride=4)]
        else:
            for k in range(2):
                packed[at, pl.ds(2 * k, 2)] = l3_ref[pl.ds((6 * edge[dw] + k) * 8 + 6 * edge[dv], 2)]
                packed[at, pl.ds(4 + 2 * k, 2)] = l2_ref[pl.ds((2 * edge[dw] + k) * 4 + 2 * edge[dv], 2)]
    pl.semaphore_wait(barrier, count - 1)

    def inside(dw, dv):
        ok = jnp.bool_(True)
        if dw < 0:
            ok = w > 0
        if dw > 0:
            ok = w < rows - 1
        if dv < 0:
            ok = ok & (v > 0)
        if dv > 0:
            ok = ok & (v < cols - 1)
        return ok

    def near_copy(dw, dv):
        out_at, in_at = (1 + dw) * 3 + 1 + dv, (1 - dw) * 3 + 1 - dv
        n = 32 if 0 in (dw, dv) else 16
        return pltpu.make_async_remote_copy(
            src_ref=packed.at[out_at, pl.ds(0, n)], dst_ref=landed.at[in_at, pl.ds(0, n)],
            send_sem=send_near.at[in_at], recv_sem=recv_near.at[in_at],
            device_id=(w + dw, v + dv), device_id_type=MESH)

    def all_copy(i, j, source):
        return pltpu.make_async_remote_copy(
            src_ref=l0_ref, dst_ref=big.at[3 + source[0], 3 + source[1]],
            send_sem=send_all.at[i * cols + j], recv_sem=recv_all.at[i * cols + j],
            device_id=(to_w[i], to_v[j]), device_id_type=MESH)

    for i, j in others:
        all_copy(i, j, (w, v)).start()
    for dw, dv in AROUND:
        @pl.when(inside(dw, dv))
        def _():
            near_copy(dw, dv).start()

    for dw, dv in AROUND:
        @pl.when(jnp.logical_not(inside(dw, dv)))
        def _():
            landed[(1 + dw) * 3 + 1 + dv] = jnp.zeros((32, width), F32)
    for r in range(rows + 6):
        for c in range(cols + 6):
            if not (3 <= r < rows + 3 and 3 <= c < cols + 3):
                big[r, c] = jnp.zeros((1, width), F32)
    big[3 + w, 3 + v] = l0_ref[...]

    lane = lax.broadcasted_iota(jnp.int32, (diag_ref.shape[1], width), 1) < half
    for s in range(diag_ref.shape[0]):
        d = diag_ref[s]
        turned = pltpu.roll(d, half, 1)
        xr[s] = jnp.where(lane, d, turned)
        xi[s] = jnp.where(lane, turned, d)
    for t in range(COARSE):
        coarse_w[t] = halves(shift_ref[t].reshape(4 * width, width))
    sign = jnp.where(lax.broadcasted_iota(jnp.int32, (1, width), 1) < half, -1.0, 1.0).astype(F32)
    odd = lax.rem(lax.broadcasted_iota(jnp.int32, (8, width), 0), 2) == 1

    def col_mask(dc, slab):
        if dc == -3:
            return jnp.where(odd, slab, 0.0)
        if dc == 3:
            return jnp.where(odd, 0.0, slab)
        return slab

    def factor(s, dr, dc):
        at = pl.ds(7 * (dr + 3) + dc + 3, 1)
        return xr[s, at, :], xi[s, at, :]

    def finish(acc_r, acc_i):
        return acc_r + sign * pltpu.roll(acc_i, half, 1)

    for r in range(8):
        win3[pl.ds((2 + r) * 24 + 8, 8)] = l3_ref[pl.ds(8 * r, 8)]
    for r in range(4):
        win2[pl.ds((2 + r) * 16 + 4, 4)] = l2_ref[pl.ds(4 * r, 4)]
    for r in range(2):
        win1[pl.ds((2 + r) * 16 + 4, 2)] = l1_ref[pl.ds(2 * r, 2)]

    def near_level(s, n, window, pitch, shifted, out):
        left = 8 if n == 8 else 4
        for dc in range(-3, 4):
            for r in range(n + 4):
                shifted[dc + 3, r] = col_mask(dc, window[pl.ds(r * pitch + left + dc, 8)])
        acc_r = [jnp.zeros((8, width), F32) for _ in range(n)]
        acc_i = [jnp.zeros((8, width), F32) for _ in range(n)]
        for dr, dc in NEAR:
            f_r, f_i = factor(s, dr, dc)
            for r in range(n):
                if allowed(dr, r % 2):
                    src = shifted[dc + 3, 2 + r + dr]
                    acc_r[r] = acc_r[r] + f_r * src
                    acc_i[r] = acc_i[r] + f_i * src
        for r in range(n):
            out[r] = finish(acc_r[r], acc_i[r])[: out.shape[1]]

    for dw, dv in AROUND:
        @pl.when(inside(dw, dv))
        def _():
            near_copy(-dw, -dv).wait_recv()

    for dw, dv in AROUND:
        at = (1 + dw) * 3 + 1 + dv
        first = lambda d, n: {-1: 0, 0: 2, 1: n + 2}[d]
        column = lambda d, n, left: {-1: left - 2, 0: left, 1: left + n}[d]
        r3, r2, r1 = first(dw, 8), first(dw, 4), first(dw, 2)
        c3, c2, c1 = column(dv, 8, 8), column(dv, 4, 4), column(dv, 2, 4)
        one_at = 24 if 0 in (dw, dv) else 8
        for k in range(2):
            win1[pl.ds((r1 + k) * 16 + c1, 2)] = landed[at, pl.ds(one_at + 2 * k, 2)]
            if dv == 0:
                win3[pl.ds((r3 + k) * 24 + c3, 8)] = landed[at, pl.ds(8 * k, 8)]
                win2[pl.ds((r2 + k) * 16 + c2, 4)] = landed[at, pl.ds(16 + 4 * k, 4)]
            elif dw == 0:
                win3[pl.ds(r3 * 24 + c3 + k, 8, stride=24)] = landed[at, pl.ds(8 * k, 8)]
                win2[pl.ds(r2 * 16 + c2 + k, 4, stride=16)] = landed[at, pl.ds(16 + 4 * k, 4)]
            else:
                win3[pl.ds((r3 + k) * 24 + c3, 2)] = landed[at, pl.ds(2 * k, 2)]
                win2[pl.ds((r2 + k) * 16 + c2, 2)] = landed[at, pl.ds(4 + 2 * k, 2)]
    near_level(4, 8, win3, 24, sh3, three_out)
    near_level(3, 4, win2, 16, sh2, two_out)
    near_level(2, 2, win1, 16, sh1, one_out)

    for i, j in others:
        all_copy(i, j, (from_w[i], from_v[j])).wait_recv()

    half_r, half_c = rows // 2, cols // 2
    for r in range(rows):
        for c in range(cols):
            q = 2 * (r % 2) + c % 2
            lhs[pl.ds((r // 2) * half_c + c // 2, 1), pl.ds(q * width, width)] = big[3 + r, 3 + c]
    boxes = half_r * half_c

    coarse = merge([lhs[:boxes, pl.ds(q * width, width)] for q in range(4)], coarse_w[1])
    grid1[:boxes] = coarse
    quarter_c = half_c // 2
    for r in range(half_r):
        for c in range(half_c):
            q = 2 * (r % 2) + c % 2
            lhs[pl.ds((r // 2) * quarter_c + c // 2, 1), pl.ds(q * width, width)] = grid1[pl.ds(r * half_c + c, 1)]
    tops = (half_r // 2) * quarter_c
    top = merge([lhs[:tops, pl.ds(q * width, width)] for q in range(4)], coarse_w[0])
    for r in range(half_r // 2):
        top_out[r] = top[r * quarter_c : (r + 1) * quarter_c]

    odd_w, odd_v = lax.rem(w, 2), lax.rem(v, 2)
    keep = {
        ("r", -3): odd_w.astype(F32), ("r", 3): (1 - odd_w).astype(F32),
        ("c", -3): odd_v.astype(F32), ("c", 3): (1 - odd_v).astype(F32),
    }
    acc_r = jnp.zeros((1, width), F32)
    acc_i = jnp.zeros((1, width), F32)
    for dr, dc in NEAR:
        f_r, f_i = factor(1, dr, dc)
        src = big[3 + w + dr, 3 + v + dc]
        if abs(dr) == 3:
            src = src * keep["r", dr]
        if abs(dc) == 3:
            src = src * keep["c", dc]
        acc_r = acc_r + f_r * src
        acc_i = acc_i + f_i * src
    zero_out[0] = finish(acc_r, acc_i)

    for r in range(half_r):
        line = []
        for c in range(half_c):
            acc_r = jnp.zeros((1, width), F32)
            acc_i = jnp.zeros((1, width), F32)
            for dr, dc in NEAR:
                if allowed(dr, r % 2) and allowed(dc, c % 2) and 0 <= r + dr < half_r and 0 <= c + dc < half_c:
                    f_r, f_i = factor(0, dr, dc)
                    src = grid1[pl.ds((r + dr) * half_c + c + dc, 1)]
                    acc_r = acc_r + f_r * src
                    acc_i = acc_i + f_i * src
            line.append(finish(acc_r, acc_i))
        coarse_out[r] = jnp.concatenate(line, axis=0)

    for dw, dv in AROUND:
        @pl.when(inside(dw, dv))
        def _():
            near_copy(dw, dv).wait_send()

    for i, j in others:
        all_copy(i, j, (w, v)).wait_send()


def write_kernel(n, *refs):
    sem = refs[2 * n]
    copies = [pltpu.make_async_copy(refs[k], refs[n + k], sem.at[k]) for k in range(n)]
    for copy in copies:
        copy.start()
    for copy in copies:
        copy.wait()


def local(mesh_shape, offsets, strengths, leaf_map, shift_matrices, transfer_diagonal):
    rows, cols = mesh_shape
    width = shift_matrices.shape[-1]
    levels = transfer_diagonal.shape[0]
    vmem = pl.BlockSpec(memory_space=pltpu.VMEM)
    boxes = (rows // 2) * (cols // 2)
    pad8 = -(-boxes // 8) * 8
    dims = (
        (SIDE * SIDE, width), (1, 1, width), (2, 2, width), (4, 4, width), (8, 8, width),
        (rows // 2, cols // 2, width), (rows // 4, cols // 4, width),
    )
    any_space = pl.BlockSpec(memory_space=pl.ANY)
    held = pl.pallas_call(
        functools.partial(tree_kernel, rows, cols, math.gcd(CHUNK, offsets.shape[-1])),
        out_shape=tuple(pltpu.VMEM(d, F32) for d in dims),
        in_specs=[vmem, vmem, vmem, any_space, any_space],
        out_specs=(vmem,) * len(dims),
        scratch_shapes=[
            pltpu.VMEM((SIDE * SIDE, 2 * width), F32),
            pltpu.VMEM(shift_matrices.shape, F32),
            pltpu.VMEM(transfer_diagonal.shape, F32),
            pltpu.VMEM((64, width), F32),
            pltpu.VMEM((16, width), F32),
            pltpu.VMEM((8, width), F32),
            pltpu.VMEM((1, width), F32),
            pltpu.SemaphoreType.DMA((2,)),
            pltpu.VMEM((9, 32, width), F32),
            pltpu.VMEM((9, 32, width), F32),
            pltpu.VMEM((rows + 6, cols + 6, 1, width), F32),
            pltpu.VMEM((12 * 24, width), F32),
            pltpu.VMEM((8 * 16, width), F32),
            pltpu.VMEM((6 * 16, width), F32),
            pltpu.VMEM((7, 12, 8, width), F32),
            pltpu.VMEM((7, 8, 8, width), F32),
            pltpu.VMEM((7, 6, 8, width), F32),
            pltpu.VMEM((levels, 49, width), F32),
            pltpu.VMEM((levels, 49, width), F32),
            pltpu.VMEM((pad8, 4 * width), F32),
            pltpu.VMEM((pad8, width), F32),
            pltpu.VMEM((COARSE, 4 * width, 2 * width), BF16),
            pltpu.SemaphoreType.DMA((rows * cols,)),
            pltpu.SemaphoreType.DMA((rows * cols,)),
            pltpu.SemaphoreType.DMA((9,)),
            pltpu.SemaphoreType.DMA((9,)),
        ],
        compiler_params=pltpu.CompilerParams(collective_id=0, has_side_effects=True),
        name="tree",
    )(offsets, strengths, leaf_map, shift_matrices, transfer_diagonal)
    n = len(dims)
    outs = pl.pallas_call(
        functools.partial(write_kernel, n),
        out_shape=tuple(jax.ShapeDtypeStruct(d, F32) for d in dims),
        in_specs=[vmem] * n,
        out_specs=(any_space,) * n,
        scratch_shapes=[pltpu.SemaphoreType.DMA((n,))],
        name="write",
    )(*[pltpu.with_memory_space_constraint(x, pltpu.VMEM) for x in held])
    return (outs[0].reshape(SIDE, SIDE, width),) + tuple(outs[1:])


def solution(mesh):
    split_2 = P("wide", "narrow", None)
    in_specs = (P(None, "wide", "narrow", None), P(None, "wide", "narrow", None), split_2, P(), P())
    out_specs = (split_2,) * 5 + (P(), P())
    body = functools.partial(local, (mesh.shape["wide"], mesh.shape["narrow"]))
    return jax.shard_map(body, mesh=mesh, in_specs=in_specs, out_specs=out_specs, check_vma=False)
```
